32 devices in a mesh: band: 4 (over x, core), grid: 8 (over z, y).
Axes of the slice: x: 2, y: 2, z: 4, core: 2. Of those that a mesh axis runs over, the one named last changes fastest.
Arguments:
- orbitals: float32 [8, 128, 128, 128], P('band', 'grid'), may hold values from -6 to 6
- occupation: float32 [8], P('band'), may hold values from 0.25 to 1
- g_list: int32 [131072], P('grid'), may hold values from 0 to 262143, as said below
- positions: float32 [3, 512], replicated, may hold values from 0 to 1
- species: int32 [512], replicated, may hold values from 0 to 3
- widths: float32 [4], replicated, may hold values from 0.3 to 2
Outputs:
- stress: float32 [3, 3], replicated
- atom_terms: float32 [512], replicated
The draws below stay inside these ranges and needn't reach their ends.
Inputs may be any that keep to these rules, and one draw needn't show every extreme that they name: `g_list`: within each aligned block of 16384 entries the values are distinct and increasing.
All inputs are finite; a program needn't handle non-finite values.
Results may differ from the reference program's by a relative error of at most 0.00013.
Values sent between devices are 32-bit elements; how exact they have to be, the bound alone decides.
A program may use at most 64 MiB of HBM per device.

```python
import math
import jax
import jax.numpy as jnp
from jax import lax

NX = 128
NY = 128
NZ = 128
GSEL_DEV = 16384
ATOMS = 512
SPECIES = 4
NBANDS = 8
SLAB_Y = 16
N_GRID = 8


def draw_orbitals(key, part):
    key_noise = jax.random.fold_in(key, 11)
    key_amplitude = jax.random.fold_in(key, 12)
    key_modes = jax.random.fold_in(key, 13)
    key_offset = jax.random.fold_in(key, 14)
    key_filter = jax.random.fold_in(key, 16)
    key_envelope = jax.random.fold_in(key, 17)
    shape = (NBANDS, NX, NY, NZ)
    noise_part = 0.3 * jnp.clip(jax.random.normal(key_noise, shape, jnp.float32), -4.0, 4.0)
    strength = jax.random.uniform(key_filter, (NBANDS,), jnp.float32, 0.04, 0.12)
    swing = jax.random.uniform(jax.random.fold_in(key_envelope, 1), (NBANDS,), jnp.float32, 0.1, 0.3)
    amp_low = 0.3
    amp_high = 0.55
    beside = jnp.roll(noise_part, 1, axis=1) + jnp.roll(noise_part, -1, axis=1)
    beside = beside + jnp.roll(noise_part, 1, axis=2) + jnp.roll(noise_part, -1, axis=2)
    beside = beside + jnp.roll(noise_part, 1, axis=3) + jnp.roll(noise_part, -1, axis=3)
    colored = noise_part + strength[:, None, None, None] * beside
    axis_x = jnp.arange(NX, dtype=jnp.float32)[None, :, None, None] / NX
    axis_y = jnp.arange(NY, dtype=jnp.float32)[None, None, :, None] / NY
    axis_z = jnp.arange(NZ, dtype=jnp.float32)[None, None, None, :] / NZ
    low_x = jax.random.randint(jax.random.fold_in(key_envelope, 2), (NBANDS,), -2, 3).astype(jnp.float32)
    low_y = jax.random.randint(jax.random.fold_in(key_envelope, 3), (NBANDS,), -2, 3).astype(jnp.float32)
    low_z = jax.random.randint(jax.random.fold_in(key_envelope, 4), (NBANDS,), -2, 3).astype(jnp.float32)
    low_phase = jax.random.uniform(jax.random.fold_in(key_envelope, 5), (NBANDS,), jnp.float32, -math.pi, math.pi)
    envelope_angle = 2.0 * math.pi * (low_x[:, None, None, None] * axis_x + low_y[:, None, None, None] * axis_y + low_z[:, None, None, None] * axis_z) + low_phase[:, None, None, None]
    envelope = 1.0 + swing[:, None, None, None] * jnp.cos(envelope_angle)
    start = (envelope * colored).astype(jnp.float32)

    def add_wave(wave, result):
        wave_key = jax.random.fold_in(key_modes, wave)
        mode_x = jax.random.randint(jax.random.fold_in(wave_key, 1), (NBANDS,), -(NX // 2), NX // 2).astype(jnp.float32)
        mode_y = jax.random.randint(jax.random.fold_in(wave_key, 2), (NBANDS,), -(NY // 2), NY // 2).astype(jnp.float32)
        mode_z = jax.random.randint(jax.random.fold_in(wave_key, 3), (NBANDS,), -(NZ // 2), NZ // 2).astype(jnp.float32)
        offset = jax.random.uniform(jax.random.fold_in(key_offset, wave), (NBANDS,), jnp.float32, -math.pi, math.pi)
        amplitude = jax.random.uniform(jax.random.fold_in(key_amplitude, wave), (NBANDS,), jnp.float32, amp_low, amp_high)
        angles = 2.0 * math.pi * (mode_x[:, None, None, None] * axis_x + mode_y[:, None, None, None] * axis_y + mode_z[:, None, None, None] * axis_z) + offset[:, None, None, None]
        return result + amplitude[:, None, None, None] * jnp.cos(angles)
    result = lax.fori_loop(0, 48, add_wave, start)
    return jnp.clip(result, -6.0, 6.0)


def draw_g_list(key, part):
    local_cells = NX * SLAB_Y * NZ
    slab_keys = jax.random.split(jax.random.fold_in(key, 21), N_GRID)

    def one_slab(slab_key):
        return jnp.sort(jax.random.permutation(slab_key, local_cells)[:GSEL_DEV])
    return jax.vmap(one_slab)(slab_keys).reshape(-1).astype(jnp.int32)


def touch_ends(values, stream_key, smallest, largest):
    longest = values.shape.index(max(values.shape))
    spots = []
    for shift in (0, 1):
        where = [jax.random.randint(jax.random.fold_in(stream_key, axis), (), 0, length) for axis, length in enumerate(values.shape)]
        where[longest] = (where[longest] + shift) % values.shape[longest]
        spots.append(tuple(where))
    return values.at[spots[0]].set(smallest).at[spots[1]].set(largest)


def shard_levels(key, extent, pieces, low, high):
    gain, own = 1.0, jax.random.fold_in(key, 6)
    for position, blocks in pieces:
        steps = jnp.exp(jax.random.uniform(jax.random.fold_in(own, position), (blocks,), jnp.float32, low / len(pieces), high / len(pieces)))
        gain = gain * jnp.repeat(steps, extent[position] // blocks).reshape([-1 if axis == position else 1 for axis in range(len(extent))])
    return gain


def setup_inputs(seed: int = 0) -> dict:
    splits = jax.random.split(jax.random.key(seed), 7)
    return {
        "orbitals": draw_orbitals(jax.random.fold_in(splits[6], 71), 0),
        "occupation": jnp.clip(0.25 + 0.75 * jax.random.uniform(splits[1], (NBANDS,), jnp.float32) ** shard_levels(splits[1], (NBANDS,), ((0, 4),), -0.2, 0.2), 0.25, 1.0),
        "g_list": draw_g_list(jax.random.fold_in(splits[6], 71), 0),
        "positions": jnp.clip(jax.random.uniform(splits[3], (3, ATOMS), jnp.float32, 0.0, 1.0), 0.0, 1.0),
        "species": touch_ends(jax.random.randint(splits[4], (ATOMS,), 0, SPECIES), jax.random.fold_in(splits[4], 1), 0, SPECIES - 1).astype(jnp.int32),
        "widths": jnp.clip(jnp.exp(jax.random.uniform(splits[5], (SPECIES,), jnp.float32, math.log(0.3), math.log(2.0))), 0.3, 2.0),
    }


HIGHEST = lax.Precision.HIGHEST


def folded_frequency(cell, length):
    folded = jnp.where(cell < length // 2, cell, cell - length)
    return folded.astype(jnp.float32)


def spectrum_sums(selected, freq_x, freq_y, freq_z, positions, species, widths, lengths, band_total):
    two_pi = 2.0 * math.pi
    wave_vector = jnp.stack([two_pi * freq_x / lengths[0], two_pi * freq_y / lengths[1], two_pi * freq_z / lengths[2]])
    wave_square = jnp.sum(wave_vector * wave_vector, axis=0)
    nonzero = (wave_square > 0).astype(jnp.float32)
    denominator = wave_square + 1.0 - nonzero
    weighted = selected * (4.0 * math.pi) * nonzero / denominator
    identity = jnp.eye(3, dtype=jnp.float32)[:, :, None]
    kernel = 2.0 * wave_vector[:, None, :] * wave_vector[None, :, :] / denominator - identity
    stress = jnp.sum(kernel * weighted[None, None, :], axis=2) / band_total
    form_factor = jnp.exp(-0.5 * wave_square[None, :] * (widths * widths)[:, None]) * weighted[None, :]
    kinds = widths.shape[0]
    one_hot = (species[:, None] == jnp.arange(kinds, dtype=jnp.int32)[None, :]).astype(jnp.float32)
    atom_count = species.shape[0]
    fractions = positions.reshape(3, atom_count // 32, 32).transpose(1, 0, 2)
    hot_rows = one_hot.reshape(atom_count // 32, 32, kinds)

    def atom_block(operands):
        fraction, hot_block = operands
        phases = two_pi * (fraction[0][:, None] * freq_x[None, :] + fraction[1][:, None] * freq_y[None, :] + fraction[2][:, None] * freq_z[None, :])
        projected = jnp.dot(jnp.cos(phases), form_factor.T, precision=HIGHEST)
        return jnp.sum(projected * hot_block, axis=1)

    atom_terms = lax.map(atom_block, (fractions, hot_rows)).reshape(atom_count) / band_total
    return stress, atom_terms


def reference(orbitals, occupation, g_list, positions, species, widths):
    cells = NX * NY * NZ

    def add_band(accumulated, operands):
        orbital_row, occupied = operands
        pair_rows = orbital_row[None] * orbitals
        spectra = jnp.fft.fftn(pair_rows, axes=(1, 2, 3)) / cells
        pair_power = jnp.real(spectra) ** 2 + jnp.imag(spectra) ** 2
        weights = occupied * occupation
        return accumulated + jnp.einsum("p,pxyz->xyz", weights, pair_power, precision=HIGHEST), None

    spectrum, ignored = lax.scan(add_band, jnp.zeros((NX, NY, NZ), jnp.float32), (orbitals, occupation))
    entries = jnp.arange(g_list.shape[0], dtype=jnp.int32)
    slab_index = entries // GSEL_DEV
    cell_x = g_list // (SLAB_Y * NZ)
    cell_y = slab_index * SLAB_Y + (g_list // NZ) % SLAB_Y
    cell_z = g_list % NZ
    selected = spectrum[cell_x, cell_y, cell_z]
    return spectrum_sums(selected, folded_frequency(cell_x, NX), folded_frequency(cell_y, NY), folded_frequency(cell_z, NZ), positions, species, widths, (NX, NY, NZ), NBANDS)
```

```python
import math

import jax
import jax.numpy as jnp
from jax import lax
from jax.sharding import PartitionSpec as P

HIGH = lax.Precision.HIGH
HIGHEST = lax.Precision.HIGHEST
TWO_PI = 2.0 * math.pi


def trig(rows, columns, length):
    products = rows[:, None] * columns[None, :] % length
    angles = TWO_PI / length * products.astype(jnp.float32)
    return jnp.cos(angles), jnp.sin(angles)


def pair_rows(own, others, band_index, band_count):
    bands = own.shape[0]
    root = math.sqrt(2.0)
    first = [own[p] * own[p] for p in range(bands)]
    first += [(root * own[p]) * own[q] for p in range(bands) for q in range(p + 1, bands)]
    stacks = [jnp.stack(first, axis=1)]
    for distance in range(1, band_count // 2 + 1):
        other = others[distance - 1]
        if 2 * distance < band_count:
            rows = [(root * own[p]) * other[q] for p in range(bands) for q in range(bands)]
        elif bands % 2 == 0:
            far = band_index >= band_count // 2
            other = jnp.where(far, jnp.roll(other, -1, axis=0), other)
            rows = [
                (root * own[p]) * other[(p + s) % bands]
                for s in range(bands // 2)
                for p in range(bands)
            ]
        else:
            rows = [own[p] * other[q] for p in range(bands) for q in range(bands)]
        stacks.append(jnp.stack(rows, axis=1))
    return stacks


def count_mask(row, lane, rows, lanes, chunk):
    steps = row.shape[0] // chunk

    def step(total, operands):
        row_part, lane_part = operands
        row_hot = (jnp.arange(rows, dtype=jnp.int32)[:, None] == row_part[None, :]).astype(jnp.bfloat16)
        lane_hot = (lane_part[:, None] == jnp.arange(lanes, dtype=jnp.int32)[None, :]).astype(jnp.bfloat16)
        return total + jnp.dot(row_hot, lane_hot, preferred_element_type=jnp.float32), None

    shaped = (row.reshape(steps, chunk), lane.reshape(steps, chunk))
    return lax.scan(step, jnp.zeros((rows, lanes), jnp.float32), shaped)[0]


def wave_tables(freq, length, position, width_of_atom):
    turns = freq[:, None] * position[None, :]
    turns = turns - jnp.round(turns)
    angles = TWO_PI * turns
    g = TWO_PI * freq / length
    damping = jnp.exp(-0.5 * (g * g)[:, None] * (width_of_atom * width_of_atom)[None, :])
    return damping * jnp.cos(angles), damping * jnp.sin(angles)


def plane_sums(density, freq_x, freq_y, freq_z, lengths, positions, width_of_atom):
    gx = TWO_PI * freq_x / lengths[0]
    gy = TWO_PI * freq_y / lengths[1]
    gz = TWO_PI * freq_z / lengths[2]
    square = (gx * gx)[:, None, None] + (gy * gy)[None, :, None] + (gz * gz)[None, None, :]
    nonzero = (square > 0).astype(jnp.float32)
    denominator = square + 1.0 - nonzero
    weighted = density * (4.0 * math.pi) * nonzero / denominator
    reduced = 2.0 * weighted / denominator
    over_x = jnp.sum(reduced, axis=(1, 2))
    over_y = jnp.sum(reduced, axis=(0, 2))
    over_z = jnp.sum(reduced, axis=(0, 1))
    flat_xy = jnp.sum(reduced, axis=2)
    lines_z = jnp.sum(reduced * gz[None, None, :], axis=2)
    total = jnp.sum(weighted)
    xx = jnp.sum(over_x * gx * gx) - total
    yy = jnp.sum(over_y * gy * gy) - total
    zz = jnp.sum(over_z * gz * gz) - total
    xy = jnp.sum(flat_xy * gx[:, None] * gy[None, :])
    xz = jnp.sum(lines_z * gx[:, None])
    yz = jnp.sum(lines_z * gy[None, :])
    stress = jnp.stack([xx, xy, xz, xy, yy, yz, xz, yz, zz]).reshape(3, 3)
    real_x, imag_x = wave_tables(freq_x, lengths[0], positions[0], width_of_atom)
    real_y, imag_y = wave_tables(freq_y, lengths[1], positions[1], width_of_atom)
    real_z, imag_z = wave_tables(freq_z, lengths[2], positions[2], width_of_atom)
    table_z = jnp.concatenate([real_z, imag_z], axis=1)
    along_z = jnp.einsum("xtz,zn->txn", weighted, table_z, precision=HIGH)
    atoms = positions.shape[1]
    real_zed, imag_zed = along_z[..., :atoms], along_z[..., atoms:]
    real_two = jnp.sum(real_zed * real_y[:, None, :] - imag_zed * imag_y[:, None, :], axis=0)
    imag_two = jnp.sum(real_zed * imag_y[:, None, :] + imag_zed * real_y[:, None, :], axis=0)
    atom_terms = jnp.sum(real_two * real_x - imag_two * imag_x, axis=0)
    return stress, atom_terms


def per_device(orbitals, occupation, g_list, positions, species, widths):
    bands, slab_x, size_y, size_z = orbitals.shape
    grid = lax.axis_size("grid")
    band_count = lax.axis_size("band")
    me = lax.axis_index("grid")
    size_x = slab_x * grid
    slab = size_y // grid
    kk = slab // 2
    half = grid // 2
    cells = float(size_x) * size_y * size_z
    low = me < half

    mate_list = lax.ppermute(g_list, "grid", [(i, grid - 1 - i) for i in range(grid)])
    edge_pairs = [(half, 0)] + [(grid - i, i) for i in range(1, half)]
    edge_list = lax.ppermute(g_list, "grid", edge_pairs)
    neighbours = [
        lax.ppermute(
            (orbitals, occupation), "band", [(i, (i + d) % band_count) for i in range(band_count)]
        )
        for d in range(1, band_count // 2 + 1)
    ]

    def scaled(pair):
        return pair[0] * jnp.sqrt(pair[1])[:, None, None, None]

    own = scaled((orbitals, occupation))
    stacks = pair_rows(own, [scaled(n) for n in neighbours], lax.axis_index("band"), band_count)

    device = jnp.arange(grid, dtype=jnp.int32)
    base = jnp.where(device < half, slab * device, slab * (grid - 1 - device) + kk)
    k_rows = (base[:, None] + jnp.arange(kk, dtype=jnp.int32)[None, :]).reshape(-1)
    cells_y = jnp.arange(size_y, dtype=jnp.int32)
    cos_y, sin_y = trig(k_rows, cells_y, size_y)
    nyquist, _ = trig(jnp.full((1,), size_y // 2, jnp.int32), cells_y, size_y)
    sin_y = jnp.where(k_rows[:, None] == 0, nyquist, sin_y)
    basis_y = jnp.stack(
        [cos_y.reshape(grid, kk, size_y), sin_y.reshape(grid, kk, size_y)], axis=1
    ) * (1.0 / cells)
    range_z = jnp.arange(size_z, dtype=jnp.int32)
    cos_z, sin_z = trig(range_z, range_z, size_z)
    range_x = jnp.arange(size_x, dtype=jnp.int32)
    cos_x, sin_x = trig(range_x, range_x, size_x)
    from_real = jnp.concatenate([cos_x, -sin_x], axis=0)
    from_imag = jnp.concatenate([sin_x, cos_x], axis=0)
    is_zero = (me == 0).astype(jnp.float32)

    def spectrum_of(stack):
        rows = jnp.einsum("gcty,xpyz->gxpctz", basis_y, stack, precision=HIGH)
        rows = lax.all_to_all(rows, "grid", split_axis=0, concat_axis=0, tiled=True)
        rows = rows.reshape(size_x, stack.shape[1], 2, kk, size_z)
        cosine, sine = rows[:, :, 0], rows[:, :, 1]
        nyquist_row = sine[:, :, :1] * is_zero
        keep = jnp.where(jnp.arange(kk) == 0, 1.0 - is_zero, 1.0)
        cosine = jnp.concatenate([cosine, nyquist_row], axis=2)
        sine = jnp.concatenate([sine * keep[:, None], jnp.zeros_like(nyquist_row)], axis=2)
        real = jnp.einsum("xptz,zm->xptm", cosine, cos_z, precision=HIGH) - jnp.einsum(
            "xptz,zm->xptm", sine, sin_z, precision=HIGH
        )
        imag = -(
            jnp.einsum("xptz,zm->xptm", cosine, sin_z, precision=HIGH)
            + jnp.einsum("xptz,zm->xptm", sine, cos_z, precision=HIGH)
        )
        both = jnp.einsum("nx,xptm->nptm", from_real, real, precision=HIGH) + jnp.einsum(
            "nx,xptm->nptm", from_imag, imag, precision=HIGH
        )
        power = jnp.sum(both * both, axis=1)
        return power[:size_x] + power[size_x:]

    spectrum = sum(spectrum_of(stack) for stack in stacks)

    chunk = math.gcd(g_list.shape[0], 1024)
    plus_list = jnp.where(low, g_list, mate_list)
    minus_list = jnp.where(low, mate_list, g_list)

    def decode(values):
        return values // (slab * size_z), values // size_z % slab, values % size_z

    def mirrored(cell, size):
        return jnp.where(cell == 0, 0, size - cell)

    x, y, z = decode(plus_list)
    t = y - jnp.where(low, 0, kk)
    row = jnp.where((t >= 0) & (t < kk), x * kk + t, -1)
    plus = count_mask(row, z, size_x * kk, size_z, chunk).reshape(size_x, kk, size_z)
    x, y, z = decode(minus_list)
    t = jnp.where(low, slab, kk) - y
    row = jnp.where((t >= 0) & (t < kk), mirrored(x, size_x) * kk + t, -1)
    minus = count_mask(row, mirrored(z, size_z), size_x * kk, size_z, chunk)
    minus = minus.reshape(size_x, kk, size_z)
    x, y, z = decode(edge_list)
    on_edge = (y == 0) & low
    is_first = me == 0
    edge_x = jnp.where(is_first, x, mirrored(x, size_x))
    edge_z = jnp.where(is_first, z, mirrored(z, size_z))
    edge = count_mask(jnp.where(on_edge, edge_x, -1), edge_z, size_x, size_z, chunk)[:, None, :]
    minus = jnp.concatenate([minus[:, :1] + edge * (1.0 - is_zero), minus[:, 1:]], axis=1)
    plus = jnp.concatenate([plus, edge * is_zero], axis=1)

    def folded(length, mirror):
        index = jnp.arange(length, dtype=jnp.int32)
        last = length // 2 if mirror else length // 2 - 1
        return jnp.where(index <= last, index, index - length).astype(jnp.float32)

    my_base = jnp.where(low, slab * me, slab * (grid - 1 - me) + kk)
    freq_y = (my_base + jnp.arange(kk, dtype=jnp.int32)).astype(jnp.float32)
    freq_y_plus = jnp.concatenate([freq_y, jnp.full((1,), -(size_y // 2), jnp.float32)])
    width_of_atom = widths[species]
    lengths = (size_x, size_y, size_z)
    stress, atoms = plane_sums(
        spectrum * plus, folded(size_x, False), freq_y_plus, folded(size_z, False),
        lengths, positions, width_of_atom,
    )
    stress_m, atoms_m = plane_sums(
        spectrum[:, :kk] * minus, folded(size_x, True), freq_y, folded(size_z, True),
        lengths, positions, width_of_atom,
    )
    total = float(bands * band_count)
    out = jnp.concatenate([(stress + stress_m).reshape(-1), atoms + atoms_m]) / total
    out = lax.psum(out, ("band", "grid"))
    return out[:9].reshape(3, 3), out[9:]


def solution(mesh):
    return jax.shard_map(
        per_device,
        mesh=mesh,
        in_specs=(P("band", "grid", None, None), P("band"), P("grid"), P(), P(), P()),
        out_specs=(P(), P()),
        check_vma=False,
    )
```

```python
import math

import functools

import jax
import jax.numpy as jnp
import numpy as np
from jax import lax
from jax.experimental import pallas as pl
from jax.experimental.pallas import tpu as pltpu
from jax.sharding import PartitionSpec as P

HIGH = lax.Precision.HIGH
HIGHEST = lax.Precision.HIGHEST
TWO_PI = 2.0 * math.pi


def trig(rows, columns, length):
    angles = TWO_PI / length * (rows[:, None] * columns[None, :] % length)
    return np.cos(angles).astype(np.float32), np.sin(angles).astype(np.float32)


def sum_kernel(axis, count, mine, total, inbox, send_sem, recv_sem):
    me = lax.axis_index(axis)
    barrier = pltpu.get_barrier_semaphore()
    mesh_ids = pl.DeviceIdType.MESH
    for p in range(1, count):
        peer = lax.rem(me + p, count)
        pl.semaphore_signal(barrier, inc=1, device_id={axis: peer}, device_id_type=mesh_ids)
    pl.semaphore_wait(barrier, count - 1)
    copies = []
    for p in range(1, count):
        copy = pltpu.make_async_remote_copy(
            src_ref=mine,
            dst_ref=inbox.at[me],
            send_sem=send_sem.at[p - 1],
            recv_sem=recv_sem.at[p - 1],
            device_id={axis: lax.rem(me + p, count)},
            device_id_type=mesh_ids,
        )
        copy.start()
        copies.append(copy)
    inbox[me] = mine[...]
    for copy in copies:
        copy.wait()
    total[...] = jnp.sum(inbox[...], axis=0)


def sum_over(block, axis, collective_id):
    count = lax.axis_size(axis)
    return pl.pallas_call(
        functools.partial(sum_kernel, axis, count),
        out_shape=jax.ShapeDtypeStruct(block.shape, block.dtype),
        in_specs=[pl.BlockSpec(memory_space=pltpu.VMEM)],
        out_specs=pl.BlockSpec(memory_space=pltpu.VMEM),
        scratch_shapes=[
            pltpu.VMEM((count,) + block.shape, block.dtype),
            pltpu.SemaphoreType.DMA((count - 1,)),
            pltpu.SemaphoreType.DMA((count - 1,)),
        ],
        compiler_params=pltpu.CompilerParams(collective_id=collective_id, has_side_effects=True),
    )(block)


def pair_rows(own, others, band_index, band_count):
    bands = own.shape[0]
    root = math.sqrt(2.0)
    first = [own[p] * own[p] for p in range(bands)]
    first += [(root * own[p]) * own[q] for p in range(bands) for q in range(p + 1, bands)]
    stacks = [jnp.stack(first, axis=1)]
    if others is None:
        return stacks
    for distance in range(1, band_count // 2 + 1):
        other = others[distance - 1]
        if 2 * distance < band_count:
            rows = [(root * own[p]) * other[q] for p in range(bands) for q in range(bands)]
        elif bands % 2 == 0:
            far = band_index >= band_count // 2
            other = jnp.where(far, jnp.roll(other, -1, axis=0), other)
            rows = [
                (root * own[p]) * other[(p + s) % bands]
                for s in range(bands // 2)
                for p in range(bands)
            ]
        else:
            rows = [own[p] * other[q] for p in range(bands) for q in range(bands)]
        stacks.append(jnp.stack(rows, axis=1))
    return stacks


def count_mask(row, lane, rows, lanes, chunk):
    steps = row.shape[0] // chunk

    def step(total, operands):
        row_part, lane_part = operands
        row_hot = (jnp.arange(rows, dtype=jnp.int32)[:, None] == row_part[None, :]).astype(jnp.bfloat16)
        lane_hot = (lane_part[:, None] == jnp.arange(lanes, dtype=jnp.int32)[None, :]).astype(jnp.bfloat16)
        return total + jnp.dot(row_hot, lane_hot, preferred_element_type=jnp.float32), None

    shaped = (row.reshape(steps, chunk), lane.reshape(steps, chunk))
    return lax.scan(step, jnp.zeros((rows, lanes), jnp.float32), shaped)[0]


def wave_tables(freq, length, position, width_of_atom):
    turns = freq[:, None] * position[None, :]
    turns = turns - jnp.round(turns)
    angles = TWO_PI * turns
    g = TWO_PI * freq / length
    damping = jnp.exp(-0.5 * (g * g)[:, None] * (width_of_atom * width_of_atom)[None, :])
    return damping * jnp.cos(angles), damping * jnp.sin(angles)


def plane_tables(mask, freq_x, freq_y, freq_z, lengths, positions, width_of_atom):
    gx = TWO_PI * freq_x / lengths[0]
    gy = TWO_PI * freq_y / lengths[1]
    gz = TWO_PI * freq_z / lengths[2]
    square = (gx * gx)[:, None, None] + (gy * gy)[None, :, None] + (gz * gz)[None, None, :]
    nonzero = (square > 0).astype(jnp.float32)
    inverse = nonzero / (square + 1.0 - nonzero)
    coulomb = mask * (4.0 * math.pi) * inverse
    real_z, imag_z = wave_tables(freq_z, lengths[2], positions[2], width_of_atom)
    table_z = jnp.concatenate([real_z, imag_z], axis=1)
    table_x = wave_tables(freq_x, lengths[0], positions[0], width_of_atom)
    table_y = wave_tables(freq_y, lengths[1], positions[1], width_of_atom)
    return coulomb, 2.0 * inverse, gx, gy, gz, table_x, table_y, table_z


def plane_sums(spectrum, tables):
    coulomb, inverse, gx, gy, gz, table_x, table_y, table_z = tables
    real_x, imag_x = table_x
    real_y, imag_y = table_y
    weighted = spectrum * coulomb
    reduced = weighted * inverse
    bx, by, bz = gx[:, None, None], gy[None, :, None], gz[None, None, :]
    total = jnp.sum(weighted)
    xx = jnp.sum(reduced * (bx * bx)) - total
    yy = jnp.sum(reduced * (by * by)) - total
    zz = jnp.sum(reduced * (bz * bz)) - total
    xy = jnp.sum(reduced * (bx * by))
    xz = jnp.sum(reduced * (bx * bz))
    yz = jnp.sum(reduced * (by * bz))
    stress = jnp.stack([xx, xy, xz, xy, yy, yz, xz, yz, zz])
    along_z = jnp.einsum("xtz,zn->txn", weighted, table_z, precision=HIGHEST)
    atoms = real_x.shape[1]
    real_zed, imag_zed = along_z[..., :atoms], along_z[..., atoms:]
    real_two = jnp.sum(real_zed * real_y[:, None, :] - imag_zed * imag_y[:, None, :], axis=0)
    imag_two = jnp.sum(real_zed * imag_y[:, None, :] + imag_zed * real_y[:, None, :], axis=0)
    atom_terms = jnp.sum(real_two * real_x - imag_two * imag_x, axis=0)
    return stress, atom_terms


def per_device(orbitals, occupation, g_list, positions, species, widths):
    bands, slab_x, size_y, size_z = orbitals.shape
    grid = lax.axis_size("grid")
    band_count = lax.axis_size("band")
    me = lax.axis_index("grid")
    size_x = slab_x * grid
    slab = size_y // grid
    kk = slab // 2
    half = grid // 2
    cells = float(size_x) * size_y * size_z
    low = me < half

    own = orbitals * jnp.sqrt(occupation)[:, None, None, None]

    device = np.arange(grid)
    base = np.where(device < half, slab * device, slab * (grid - 1 - device) + kk)
    k_rows = (base[:, None] + np.arange(kk)[None, :]).reshape(-1)
    cells_y = np.arange(size_y)
    cos_y, sin_y = trig(k_rows, cells_y, size_y)
    nyquist, _ = trig(np.full((1,), size_y // 2), cells_y, size_y)
    sin_y = np.where(k_rows[:, None] == 0, nyquist, sin_y)
    basis_y = np.stack(
        [cos_y.reshape(grid, kk, size_y), sin_y.reshape(grid, kk, size_y)], axis=1
    ) * np.float32(1.0 / cells)
    range_z = np.arange(size_z)
    cos_z, sin_z = trig(range_z, range_z, size_z)
    range_x = np.arange(size_x)
    cos_x, sin_x = trig(range_x, range_x, size_x)
    from_real = np.concatenate([cos_x, -sin_x], axis=0)
    from_imag = np.concatenate([sin_x, cos_x], axis=0)
    is_zero = (me == 0).astype(jnp.float32)

    def along_y(stack):
        return jnp.einsum("gcty,xpyz->gxpctz", basis_y, stack, precision=HIGH)

    def exchanged(rows):
        return lax.all_to_all(rows, "grid", split_axis=0, concat_axis=0, tiled=True)

    def spectrum_of(rows):
        rows = rows.reshape(size_x, rows.shape[2], 2, kk, size_z)
        cosine, sine = rows[:, :, 0], rows[:, :, 1]
        nyquist_row = sine[:, :, :1] * is_zero
        keep = jnp.where(jnp.arange(kk) == 0, 1.0 - is_zero, 1.0)
        cosine = jnp.concatenate([cosine, nyquist_row], axis=2)
        sine = jnp.concatenate([sine * keep[:, None], jnp.zeros_like(nyquist_row)], axis=2)
        real = jnp.einsum("xptz,zm->xptm", cosine, cos_z, precision=HIGH) - jnp.einsum(
            "xptz,zm->xptm", sine, sin_z, precision=HIGH
        )
        imag = -(
            jnp.einsum("xptz,zm->xptm", cosine, sin_z, precision=HIGH)
            + jnp.einsum("xptz,zm->xptm", sine, cos_z, precision=HIGH)
        )
        both = jnp.einsum("nx,xptm->nptm", from_real, real, precision=HIGH) + jnp.einsum(
            "nx,xptm->nptm", from_imag, imag, precision=HIGH
        )
        power = jnp.sum(both * both, axis=1)
        return power[:size_x] + power[size_x:]

    band_index = lax.axis_index("band")
    ready = along_y(pair_rows(own, None, band_index, band_count)[0])
    ready, own, g_list = lax.optimization_barrier((ready, own, g_list))
    arrived = [exchanged(ready)]
    neighbours = [
        lax.ppermute(own, "band", [(i, (i + d) % band_count) for i in range(band_count)])
        for d in range(1, band_count // 2 + 1)
    ]
    mate_list = lax.ppermute(g_list, "grid", [(i, grid - 1 - i) for i in range(grid)])
    edge_pairs = [(half, 0)] + [(grid - i, i) for i in range(1, half)]
    edge_list = lax.ppermute(g_list, "grid", edge_pairs)
    stacks = pair_rows(own, neighbours, band_index, band_count)

    chunk = math.gcd(g_list.shape[0], 1024)
    plus_list = jnp.where(low, g_list, mate_list)
    minus_list = jnp.where(low, mate_list, g_list)

    def decode(values):
        return values // (slab * size_z), values // size_z % slab, values % size_z

    def mirrored(cell, size):
        return jnp.where(cell == 0, 0, size - cell)

    x, y, z = decode(plus_list)
    t = y - jnp.where(low, 0, kk)
    row = jnp.where((t >= 0) & (t < kk), x * kk + t, -1)
    plus = count_mask(row, z, size_x * kk, size_z, chunk).reshape(size_x, kk, size_z)
    x, y, z = decode(minus_list)
    t = jnp.where(low, slab, kk) - y
    row = jnp.where((t >= 0) & (t < kk), mirrored(x, size_x) * kk + t, -1)
    minus = count_mask(row, mirrored(z, size_z), size_x * kk, size_z, chunk)
    minus = minus.reshape(size_x, kk, size_z)
    x, y, z = decode(edge_list)
    on_edge = (y == 0) & low
    is_first = me == 0
    edge_x = jnp.where(is_first, x, mirrored(x, size_x))
    edge_z = jnp.where(is_first, z, mirrored(z, size_z))
    edge = count_mask(jnp.where(on_edge, edge_x, -1), edge_z, size_x, size_z, chunk)[:, None, :]
    minus = jnp.concatenate([minus[:, :1] + edge * (1.0 - is_zero), minus[:, 1:]], axis=1)
    plus = jnp.concatenate([plus, edge * is_zero], axis=1)

    def folded(length, mirror):
        index = jnp.arange(length, dtype=jnp.int32)
        last = length // 2 if mirror else length // 2 - 1
        return jnp.where(index <= last, index, index - length).astype(jnp.float32)

    my_base = jnp.where(low, slab * me, slab * (grid - 1 - me) + kk)
    freq_y = (my_base + jnp.arange(kk, dtype=jnp.int32)).astype(jnp.float32)
    freq_y_plus = jnp.concatenate([freq_y, jnp.full((1,), -(size_y // 2), jnp.float32)])
    width_of_atom = widths[species]
    lengths = (size_x, size_y, size_z)
    plus_tables = plane_tables(
        plus, folded(size_x, False), freq_y_plus, folded(size_z, False),
        lengths, positions, width_of_atom,
    )
    minus_tables = plane_tables(
        minus, folded(size_x, True), freq_y, folded(size_z, True),
        lengths, positions, width_of_atom,
    )

    spectrum = 0.0
    for index, stack in enumerate(stacks[1:]):
        rows, held = along_y(stack), arrived[-1]
        if index == len(stacks) - 2:
            rows, held, plus_tables, minus_tables = lax.optimization_barrier(
                (rows, held, plus_tables, minus_tables)
            )
        else:
            rows, held = lax.optimization_barrier((rows, held))
        arrived.append(exchanged(rows))
        spectrum = spectrum + spectrum_of(held)
    spectrum = spectrum + spectrum_of(arrived[-1])
    stress, atoms = plane_sums(spectrum, plus_tables)
    stress_m, atoms_m = plane_sums(spectrum[:, :kk], minus_tables)
    total = float(bands * band_count)
    out = jnp.concatenate([stress + stress_m, atoms + atoms_m]) / total
    size = out.shape[0]
    padded = -(-size // 1024) * 1024
    block = jnp.pad(out, (0, padded - size)).reshape(padded // 128, 128)
    out = sum_over(sum_over(block, "grid", 0), "band", 1).reshape(-1)[:size]
    return out[:9].reshape(3, 3), out[9:]


def solution(mesh):
    return jax.shard_map(
        per_device,
        mesh=mesh,
        in_specs=(P("band", "grid", None, None), P("band"), P("grid"), P(), P(), P()),
        out_specs=(P(), P()),
        check_vma=False,
    )
```
